32 devices in a mesh: rep: 2 (over y), tp: 4 (over z), sub: 4 (over x, core).
Axes of the slice: x: 2, y: 2, z: 4, core: 2. Of those that a mesh axis runs over, the one named last changes fastest.
Arguments:
- hidden_in: bfloat16 [128, 6144], P(('rep', 'sub'), 'tp'), parts along dimension 0, may hold values from -128 to 128
- query: bfloat16 [128, 6144], P(('rep', 'sub'), 'tp'), parts along dimension 0, may hold values from -128 to 128
- key_new: bfloat16 [128, 1024], P(('rep', 'sub'), 'tp'), parts along dimension 0, may hold values from -8 to 8
- value_new: bfloat16 [128, 1024], P(('rep', 'sub'), 'tp'), parts along dimension 0, may hold values from -6 to 6
- key_cache: bfloat16 [128, 128, 1024], P(('rep', 'sub'), 'tp'), parts along dimension 0, may hold values from -8 to 8
- value_cache: bfloat16 [128, 128, 1024], P(('rep', 'sub'), 'tp'), parts along dimension 0, may hold values from -6 to 6
- lengths: int32 [128], P(('rep', 'sub')), parts along dimension 0, may hold values from 2 to 128
- out_weight: bfloat16 [6144, 6144], P('sub', 'tp'), may hold values from -0.078125 to 0.078125
- norm_gain: bfloat16 [6144], P('tp'), may hold values from 0.099609375 to 1.8984375
- router_weight: bfloat16 [6144, 4], P('tp'), may hold values from -0.078125 to 0.078125
- routes: int32 [128, 2], P(('rep', 'sub')), parts along dimension 0, may hold values from 0 to 3, all different within a row; in each aligned block of 16 rows (0 to 15, 16 to 31, ...) at most 12 rows name the same one
- gate_weight: bfloat16 [4, 6144, 8192], P('sub', None, 'tp'), may hold values from -0.078125 to 0.078125
- up_weight: bfloat16 [4, 6144, 8192], P('sub', None, 'tp'), may hold values from -0.078125 to 0.078125
- down_weight: bfloat16 [4, 8192, 6144], P('sub', 'tp'), may hold values from -0.09375 to 0.09375
Outputs:
- layer_out: bfloat16 [128, 6144], P(('rep', 'sub'), 'tp'), parts along dimension 0
The draws below stay inside these ranges and needn't reach their ends.
There are 2 independent parts, one for each index of `rep`. The reference program is written for one: setup_inputs(seed, part) draws one part's arguments, and reference() takes and returns one part's arrays. A program takes and returns all parts, laid end to end along the dimension named above; an argument that names none is the same for every part. Nothing has to cross between parts.
Inputs may be any that keep to these rules, and one draw needn't show every extreme that they name: `routes`: the two experts of a row differ; within the 16 rows of one index of sub, no expert is named by more than 12 rows, a bound that some such block reaches.
All inputs are finite; a program needn't handle non-finite values.
Results may differ from the reference program's by a relative error of at most 0.0075.
Values may be sent and summed in bfloat16 or wider, within the bound.
A program may use at most 128 MiB of HBM per device.

```python
import math
import jax
import jax.numpy as jnp
import numpy as np
from jax import lax

D = 6144
H = 48
KVH = 8
HD = 128
FF = 8192
E = 4
SEQ_SUB = 16
B = 64
CACHE = 128
MOST = 12


def draw_query(key, part):
    noise = jnp.clip(jax.random.normal(jax.random.fold_in(key, 1), (B, H * HD), jnp.float32), -6.0, 6.0)
    return noise.astype(jnp.bfloat16)


def draw_key_cache(key, part):
    noise = jnp.clip(jax.random.normal(jax.random.fold_in(key, 2), (B, CACHE, KVH * HD), jnp.float32), -6.0, 6.0)
    return noise.astype(jnp.bfloat16)


def draw_key_new(key, part):
    noise = jnp.clip(jax.random.normal(jax.random.fold_in(key, 3), (B, KVH * HD), jnp.float32), -6.0, 6.0)
    return noise.astype(jnp.bfloat16)


def draw_hidden_in(key, part):
    noise = jnp.clip(jax.random.normal(jax.random.fold_in(key, 4), (B, D), jnp.float32), -6.0, 6.0)
    column = jnp.arange(D).astype(jnp.float32)
    noise = noise * jnp.sqrt(1.0 + 2.0 * column / D)[None, :]
    return noise.astype(jnp.bfloat16)


def plant(values, rng, least, largest):
    longest = values.shape.index(max(values.shape))
    spots = []
    for shift in (0, 1):
        where = [jax.random.randint(jax.random.fold_in(rng, axis), (), 0, length) for axis, length in enumerate(values.shape)]
        where[longest] = (where[longest] + shift) % values.shape[longest]
        spots.append(tuple(where))
    return values.at[spots[0]].set(least).at[spots[1]].set(largest)


def strengthened(entries, own_key, source, target, parts, factor):
    owner, partner = [(jnp.arange(entries.shape[axis_at]) // (entries.shape[axis_at] // parts)).reshape([-1 if axis == axis_at else 1 for axis in range(entries.ndim)]) for axis_at in (source, target)]
    chosen = jax.random.permutation(own_key, parts)[partner]
    strong = (owner == chosen) | (owner == (partner + parts // 2) % parts)
    return jnp.where(strong, factor * entries, entries)


def level_of(key, dims, cuts, low, top_value):
    factor_of, own = 1.0, jax.random.fold_in(key, 6)
    for position, shards_of in cuts:
        draws = jnp.exp(jax.random.uniform(jax.random.fold_in(own, position), (shards_of,), jnp.float32, low / len(cuts), top_value / len(cuts)))
        factor_of = factor_of * jnp.repeat(draws, dims[position] // shards_of).reshape([-1 if axis == position else 1 for axis in range(len(dims))])
    return factor_of


def deal_out(key, own, number, rows, amount, top, most, slope):
    order = jax.random.permutation(key, amount)
    heavy_load, usual = shares(amount, rows * top, most, slope, True), shares(amount, rows * top, most, slope, False)
    places = jnp.arange(amount)

    def named(sizes, rotation):
        used = int((sizes > 0).sum())
        fixed = max(1, used // 4)
        passed = fixed + (places - fixed + rotation * (used - fixed)) % max(1, amount - fixed)
        return jnp.zeros((amount,), jnp.int32).at[order[jnp.where(places < fixed, places, passed)]].set(jnp.asarray(sizes, jnp.int32))

    sizes = jnp.where(number % 4 == 0, named(heavy_load, number // 4), named(usual, number - number // 4 - 1))
    mixed = jax.random.permutation(jax.random.fold_in(own, 3), amount)
    source_of, receiver = mixed[0:amount // 2 * 2:2], mixed[1:amount // 2 * 2:2]
    margin = jnp.minimum(sizes[source_of] - 1, most - sizes[receiver]) // 2
    margin = jnp.where((source_of == order[0]) | (receiver == order[0]) | (sizes[receiver] == 0), 0, jnp.maximum(margin, 0))
    passed = jax.random.randint(jax.random.fold_in(own, 4), (amount // 2,), 0, 1 << 20) % (margin + 1)
    sizes = sizes.at[source_of].add(-passed).at[receiver].add(passed)
    labels = jnp.searchsorted(jnp.cumsum(sizes), jnp.arange(rows * top), side="right").astype(jnp.int32)
    grid = labels.reshape(top, rows).T
    grid = grid[jax.random.permutation(jax.random.fold_in(own, 1), rows)]
    rotation = jax.random.randint(jax.random.fold_in(own, 2), (rows, 1), 0, top)
    return jnp.take_along_axis(grid, (jnp.arange(top)[None, :] + rotation) % top, axis=1)


def shares(number_of, total, bound, slope, full):
    loads = [(1 << 20) // math.isqrt(standing ** slope) + 1 for standing in range(1, number_of + 1)]
    largest = bound if full else min(bound, max(-(-total // number_of), total * loads[0] // sum(loads)))
    least = 1 if total - largest >= number_of - 1 else 0
    given, rest = [largest] + [least] * (number_of - 1), total - largest - least * (number_of - 1)
    while rest > 0:
        candidates = [i for i in range(1, number_of) if given[i] < largest] or [i for i in range(1, number_of) if given[i] < bound]
        mass, remaining = sum([loads[i] for i in candidates]), rest
        for i in candidates:
            addition = min(bound - given[i], max(1, remaining * loads[i] // mass), rest)
            given[i] = given[i] + addition
            rest = rest - addition
    return np.array(given)


def gaussian(own_key, dims, spread, bound, shards=(), held_as=jnp.bfloat16):
    array = spread * jax.random.normal(own_key, dims, jnp.float32)
    if shards:
        array = array * level_of(own_key, dims, shards, -0.22, 0.18)
    return jnp.clip(array, -bound, bound).astype(held_as)


def noise_with(own_key, dims, spread, reach, shards, heavy, kind=jnp.bfloat16):
    entries = spread * jax.random.normal(own_key, dims, jnp.float32)
    if shards:
        entries = entries * level_of(own_key, dims, shards, -0.22, 0.18)
    return jnp.clip(strengthened(entries, jax.random.fold_in(own_key, 3), *heavy), -reach, reach).astype(kind)


def setup_inputs(seed: int = 0, part: int = 0) -> dict:
    seeds = jax.random.split(jax.random.key(seed), 15)
    part_splits = jax.random.split(jax.random.fold_in(seeds[14], part), 15)
    hidden_in = draw_hidden_in(jax.random.fold_in(jax.random.fold_in(seeds[14], part), 71), part)
    query = draw_query(jax.random.fold_in(jax.random.fold_in(seeds[14], part), 71), part)
    key_new = draw_key_new(jax.random.fold_in(jax.random.fold_in(seeds[14], part), 71), part)
    value_new = gaussian(part_splits[3], (B, KVH * HD), 1.0, 6.0, ((0, 4), (1, 4)))
    key_cache = draw_key_cache(jax.random.fold_in(jax.random.fold_in(seeds[14], part), 71), part)
    value_cache = gaussian(part_splits[5], (B, CACHE, KVH * HD), 1.0, 6.0, ((0, 4), (1, 4)))
    lengths = plant(jax.random.randint(part_splits[6], (B,), 2, CACHE + 1), jax.random.fold_in(part_splits[6], 1), 2, CACHE).astype(jnp.int32)
    out_weight = gaussian(seeds[7], (H * HD, D), (H * HD) ** -0.5, 0.078125, ((0, 4), (1, 4)))
    norm_gain = jnp.clip(1.0 + 0.18 * jax.random.normal(seeds[8], (D,), jnp.float32), 0.099609375, 1.8984375).astype(jnp.bfloat16)
    router_weight = gaussian(seeds[9], (D, E), D ** -0.5, 0.078125, ((0, 4),))
    routes_keys = jax.random.split(jax.random.fold_in(part_splits[10], 1), B // SEQ_SUB)
    routes_turns = jax.random.permutation(jax.random.fold_in(part_splits[10], 3), B // SEQ_SUB)
    routes = jax.vmap(lambda own, number: deal_out(jax.random.fold_in(part_splits[10], 2), own, number, SEQ_SUB, E, 2, MOST, 2))(routes_keys, routes_turns).reshape((B, 2))
    gate_weight = gaussian(seeds[11], (E, D, FF), D ** -0.5, 0.078125, ((0, 4), (2, 4)))
    up_weight = gaussian(seeds[12], (E, D, FF), D ** -0.5, 0.078125, ((0, 4), (2, 4)))
    down_weight = noise_with(seeds[13], (E, FF, D), FF ** -0.5, 0.09375, ((0, 4), (1, 4)), (1, 2, 4, 2.0))
    return dict(hidden_in=hidden_in, query=query, key_new=key_new, value_new=value_new, key_cache=key_cache, value_cache=value_cache, lengths=lengths, out_weight=out_weight, norm_gain=norm_gain, router_weight=router_weight, routes=routes, gate_weight=gate_weight, up_weight=up_weight, down_weight=down_weight)


def reference(hidden_in, query, key_new, value_new, key_cache, value_cache, lengths, out_weight, norm_gain, router_weight, routes, gate_weight, up_weight, down_weight):
    group_size = H // KVH
    scale_factor = 1.0 / HD ** 0.5
    query_rows = query.astype(jnp.float32).reshape(B, KVH, group_size, HD)
    cached_keys = key_cache.astype(jnp.float32).reshape(B, CACHE, KVH, HD)
    cached_values = value_cache.astype(jnp.float32).reshape(B, CACHE, KVH, HD)
    scores = jnp.einsum('bkgd,bpkd->bkgp', query_rows, cached_keys) * scale_factor
    valid = jnp.arange(CACHE, dtype=jnp.int32)[None, :] < lengths[:, None]
    scores = jnp.where(valid[:, None, None, :], scores, -jnp.inf)
    fresh_keys = key_new.astype(jnp.float32).reshape(B, KVH, HD)
    new_values = value_new.astype(jnp.float32).reshape(B, KVH, HD)
    owned_part = jnp.einsum('zyqn,zyn->zyq', query_rows, fresh_keys) * scale_factor
    run_max = jnp.maximum(lax.optimization_barrier(jnp.max(scores, axis=-1)), owned_part)
    weights = jnp.exp(scores - run_max[..., None])
    own_weight = jnp.exp(owned_part - run_max)
    total = lax.optimization_barrier(jnp.sum(weights, axis=-1)) + own_weight
    summed = jnp.einsum('bkgp,bpkd->bkgd', weights, cached_values) + own_weight[..., None] * new_values[:, :, None, :]
    attn = (summed / total[..., None]).reshape(B, H * HD).astype(jnp.bfloat16)
    resid = hidden_in.astype(jnp.float32) + jnp.dot(attn, out_weight, preferred_element_type=jnp.float32)
    root = jnp.sqrt(lax.optimization_barrier(jnp.mean(resid * resid, axis=-1, keepdims=True)) + 1e-05)
    normed = resid / root * norm_gain.astype(jnp.float32)
    normed_low = normed.astype(jnp.bfloat16)
    logits = jnp.dot(normed, router_weight.astype(jnp.float32), precision=lax.Precision.HIGHEST)
    expert_ids = jnp.arange(E, dtype=jnp.int32)[None, :]
    first_hot = (routes[:, 0:1] == expert_ids).astype(jnp.float32)
    second_hot = (routes[:, 1:2] == expert_ids).astype(jnp.float32)
    first_logit = lax.optimization_barrier(jnp.sum(logits * first_hot, axis=-1))
    second_logit = lax.optimization_barrier(jnp.sum(logits * second_hot, axis=-1))
    first_weight = 1.0 / (1.0 + jnp.exp(second_logit - first_logit))
    second_weight = 1.0 / (1.0 + jnp.exp(first_logit - second_logit))
    dense = first_weight[:, None] * first_hot + second_weight[:, None] * second_hot
    mixed = jnp.zeros((B, D), jnp.float32)
    for expert in range(E):
        gate_out = jnp.dot(normed_low, gate_weight[expert], preferred_element_type=jnp.float32)
        up_out = jnp.dot(normed_low, up_weight[expert], preferred_element_type=jnp.float32)
        inner = (jax.nn.silu(gate_out) * up_out).astype(jnp.bfloat16)
        result = jnp.dot(inner, down_weight[expert], preferred_element_type=jnp.float32)
        mixed = mixed + dense[:, expert:expert + 1] * result
    return (resid + mixed).astype(jnp.bfloat16)
```

```python
import functools

import jax
import jax.numpy as jnp
import numpy as np
from jax import lax
from jax.experimental import pallas as pl
from jax.experimental.pallas import tpu as pltpu
from jax.sharding import PartitionSpec as P

D = 6144
H = 48
KVH = 8
HD = 128
E = 4


def combined_all(value, axis, combine):
    everything = jax.tree.map(lambda part: lax.all_gather(part, axis), value)
    first = jax.tree.map(lambda part: part[0], everything)

    def hop(k, so_far):
        return combine(so_far, jax.tree.map(lambda part: part[k], everything))

    return lax.fori_loop(1, lax.axis_size(axis), hop, first)


def join_softmax(first, second):
    joined = jnp.maximum(first[0], second[0])
    first_scale = jnp.exp(first[0] - joined)
    second_scale = jnp.exp(second[0] - joined)
    totals = first[1] * first_scale + second[1] * second_scale
    summed = first[2] * first_scale[..., None] + second[2] * second_scale[..., None]
    return (joined, totals, summed)


def on_device(
    hidden_in,
    query,
    key_new,
    value_new,
    key_cache,
    value_cache,
    lengths,
    out_weight,
    norm_gain,
    router_weight,
    routes,
    gate_weight,
    up_weight,
    down_weight,
):
    seq_rows = hidden_in.shape[0]
    feat_width = hidden_in.shape[1]
    group_size = H // KVH
    scale_factor = 1.0 / HD**0.5
    local_len = key_cache.shape[1]
    all_query, all_key, all_value = (
        lax.all_gather(query, "tp", axis=1, tiled=True),
        lax.all_gather(key_new, "tp", axis=1, tiled=True),
        lax.all_gather(value_new, "tp", axis=1, tiled=True),
    )
    query_rows = all_query.reshape(seq_rows, KVH, group_size, HD)
    cached_keys = key_cache.reshape(seq_rows, local_len, KVH, HD)
    cached_values = value_cache.reshape(seq_rows, local_len, KVH, HD).astype(jnp.float32)
    scores = (
        jnp.einsum("bkgd,bpkd->bkgp", query_rows, cached_keys, preferred_element_type=jnp.float32)
        * scale_factor
    )
    positions = lax.axis_index("tp") * local_len + jnp.arange(local_len, dtype=jnp.int32)
    valid = positions[None, :] < lengths[:, None]
    scores = jnp.where(valid[:, None, None, :], scores, -jnp.inf)
    owned_part = (
        jnp.einsum(
            "zyqn,zyn->zyq",
            query_rows,
            all_key.reshape(seq_rows, KVH, HD),
            preferred_element_type=jnp.float32,
        )
        * scale_factor
    )
    local_max = jnp.maximum(jnp.max(scores, axis=-1), owned_part)
    weights = jnp.exp(scores - local_max[..., None])
    partial_total = jnp.sum(weights, axis=-1)
    local_summed = jnp.einsum("bkgp,bpkd->bkgd", weights, cached_values)
    run_max, total, summed = combined_all(
        (local_max, partial_total, local_summed), "tp", join_softmax
    )
    own_weight = jnp.exp(owned_part - run_max)
    total = total + own_weight
    new_values = all_value.reshape(seq_rows, KVH, 1, HD).astype(jnp.float32)
    summed = summed + own_weight[..., None] * new_values
    attn = (summed / total[..., None]).reshape(seq_rows, H * HD).astype(jnp.bfloat16)
    all_rows_attn = lax.all_to_all(attn, "sub", split_axis=1, concat_axis=0, tiled=True)
    partial_proj = jnp.dot(all_rows_attn, out_weight, preferred_element_type=jnp.float32)
    projected = lax.psum_scatter(partial_proj, "sub", scatter_dimension=0, tiled=True)
    resid = hidden_in.astype(jnp.float32) + projected
    gain_full = norm_gain.astype(jnp.float32)[None, :]
    router_full = router_weight.astype(jnp.float32)
    squares = lax.psum(jnp.sum(resid * resid, axis=-1), "tp")
    root = jnp.sqrt(squares / D + 1e-05)
    normed = resid / root[:, None] * gain_full
    logits = lax.psum(jnp.dot(normed, router_full, precision=lax.Precision.HIGHEST), "tp")
    normed_low = normed.astype(jnp.bfloat16)
    expert_ids = jnp.arange(E, dtype=jnp.int32)[None, :]
    first_hot = (routes[:, 0:1] == expert_ids).astype(jnp.float32)
    second_hot = (routes[:, 1:2] == expert_ids).astype(jnp.float32)
    first_logit = jnp.sum(logits * first_hot, axis=-1)
    second_logit = jnp.sum(logits * second_hot, axis=-1)
    first_weight = 1.0 / (1.0 + jnp.exp(second_logit - first_logit))
    second_weight = 1.0 / (1.0 + jnp.exp(first_logit - second_logit))
    dense = first_weight[:, None] * first_hot + second_weight[:, None] * second_hot
    gate_local = gate_weight[0]
    up_local = up_weight[0]
    down_local = down_weight[0]
    every_row = lax.all_gather(normed_low, "sub", axis=0, tiled=True)
    piece = lax.all_gather(every_row, "tp", axis=1, tiled=True)
    gate_out = jnp.dot(piece, gate_local, preferred_element_type=jnp.float32)
    up_out = jnp.dot(piece, up_local, preferred_element_type=jnp.float32)
    inner = (jax.nn.silu(gate_out) * up_out).astype(jnp.bfloat16)
    result = jnp.dot(inner, down_local, preferred_element_type=jnp.float32)
    outputs = lax.psum_scatter(result, "tp", scatter_dimension=1, tiled=True)
    returned = lax.all_to_all(outputs, "sub", split_axis=0, concat_axis=0, tiled=True)
    returned = returned.reshape(E, seq_rows, feat_width)
    mixed = jnp.einsum("erc,re->rc", returned, dense)
    return (resid + mixed).astype(jnp.bfloat16)


MESH = pl.DeviceIdType.MESH
HP = 16
KC = 512
NEG = -1e30


def layer_kernel(
    n,
    len_ref, q_ref, kn_ref, vn_ref, hid_ref, gain_ref, rt_ref, routes_ref, kvm_ref, pos_ref, own_ref,
    kc_hbm, vc_hbm, ow_hbm, gw_hbm, uw_hbm, dw_hbm,
    out_ref,
    slots, kc, vc, q_all, o_send, o_recv, st_send, st_recv, att, attn_all, attn_sub,
    pr_send, pr_recv, resid, hs_send, hs_recv, x_all, f_all, gacc, uacc, inner,
    y_send, y_recv, z_send, z_recv,
    slot_sem, kv_sem, send_sem, recv_sem,
):
    t = lax.axis_index("tp")
    s = lax.axis_index("sub")
    rows, feat = hid_ref.shape
    local_len = kc.shape[1]
    kvh = kc.shape[2] // HD
    hc = feat // HD
    ff = slots.shape[2]
    n_slots = slots.shape[0]
    per_feat = feat // KC
    n_up = n * per_feat
    k_down = ff // KC
    n_down = n * k_down
    f32, bf16 = jnp.float32, jnp.bfloat16

    def up(d, i):
        return lax.rem(i + d, n)

    def down(d, i):
        return lax.rem(i + n - d, n)

    kcopy = pltpu.make_async_copy(kc_hbm, kc, kv_sem.at[0])
    vcopy = pltpu.make_async_copy(vc_hbm, vc, kv_sem.at[1])
    kcopy.start()
    vcopy.start()

    def ow_copy(i):
        slot = n_slots - per_feat + i
        return pltpu.make_async_copy(
            ow_hbm.at[pl.ds(i * KC, KC), :], slots.at[slot, :, pl.ds(0, feat)], slot_sem.at[slot]
        )

    def up_copy(hbm, k, which):
        block, part = k // per_feat, lax.rem(k, per_feat)
        row = pl.multiple_of(up(block, t) * feat + part * KC, KC)
        return pltpu.make_async_copy(
            hbm.at[0, pl.ds(row, KC), :], slots.at[2 * k + which], slot_sem.at[2 * k + which]
        )

    def down_copy(j):
        block, part = j // k_down, lax.rem(j, k_down)
        slot = lax.rem(j + n_slots - per_feat, n_slots)
        col = pl.multiple_of(up(block + 1, t) * feat, 128)
        row = pl.multiple_of(part * KC, KC)
        return pltpu.make_async_copy(
            dw_hbm.at[0, pl.ds(row, KC), pl.ds(col, feat)],
            slots.at[slot, :, pl.ds(0, feat)],
            slot_sem.at[slot],
        )

    for i in range(per_feat):
        ow_copy(i).start()

    @pl.loop(0, n_up)
    def _(k):
        up_copy(gw_hbm, k, 0).start()
        up_copy(uw_hbm, k, 1).start()

    barrier = pltpu.get_barrier_semaphore()
    for d in range(1, n):
        pl.semaphore_signal(barrier, inc=1, device_id={"tp": up(d, t)}, device_id_type=MESH)
        pl.semaphore_signal(barrier, inc=1, device_id={"sub": up(d, s)}, device_id_type=MESH)
    pl.semaphore_wait(barrier, 2 * (n - 1))

    def remote(stage, source, target, axis, peer, key, lane, who):
        return pltpu.make_async_remote_copy(
            src_ref=source,
            dst_ref=target,
            send_sem=send_sem.at[stage, key, lane],
            recv_sem=recv_sem.at[stage, who, lane],
            device_id={axis: peer},
            device_id_type=MESH,
        )

    pending = []

    def send(stage, source, target, axis, d, lane=0):
        me = t if axis == "tp" else s
        copy = remote(stage, source, target, axis, up(d, me), d, lane, me)
        copy.start()
        pending.append(copy)

    def arrive(stage, target, axis, who, lane=0):
        remote(stage, target, target, axis, who, 0, lane, who).wait_recv()

    for d in range(1, n):
        send(0, q_ref, q_all.at[t], "tp", d)
    q_all[t] = q_ref[...]
    kcopy.wait()
    vcopy.wait()
    for d in range(1, n):
        arrive(0, q_all.at[down(d, t)], "tp", down(d, t))

    lanes = lax.broadcasted_iota(jnp.int32, (n * HP, 128), 1)
    scale = 1.0 / HD**0.5
    kvm = kvm_ref[...] > 0.5
    positions = pos_ref[...] + t * local_len
    own_ok = own_ref[...] == t

    def per_row(b, carry):
        mx, tot = carry
        q = q_all[:, b].reshape(n * HP, HD)
        krow, vrow = kc[b], vc[b]
        keys = jnp.concatenate([krow[:, g * HD : (g + 1) * HD] for g in range(kvh)], axis=0)
        vals = jnp.concatenate([vrow[:, g * HD : (g + 1) * HD] for g in range(kvh)], axis=0)
        dims = (((1,), (1,)), ((), ()))
        sc = lax.dot_general(q, keys, dims, preferred_element_type=f32) * scale
        so = lax.dot_general(q, kn_ref[b], dims, preferred_element_type=f32) * scale
        ok = jnp.logical_and(kvm, positions < len_ref[b])
        sc = jnp.where(ok, sc, NEG)
        so = jnp.where(own_ok, so, NEG)
        m = jnp.maximum(jnp.max(sc, axis=1, keepdims=True), jnp.max(so, axis=1, keepdims=True))
        p = jnp.where(ok, jnp.exp(sc - m), 0.0)
        po = jnp.where(own_ok, jnp.exp(so - m), 0.0)
        l = jnp.sum(p, axis=1, keepdims=True) + jnp.sum(po, axis=1, keepdims=True)
        o = jnp.dot(p.astype(bf16), vals, preferred_element_type=f32)
        o = o + jnp.dot(po.astype(bf16), vn_ref[b], preferred_element_type=f32)
        o_send[:, b] = o.astype(bf16).reshape(n, HP, HD)
        return jnp.where(lanes == b, m, mx), jnp.where(lanes == b, l, tot)

    zero = jnp.zeros((n * HP, 128), f32)
    mx, tot = lax.fori_loop(0, rows, per_row, (zero, zero))
    st_send[:, 0] = mx.reshape(n, HP, 128)
    st_send[:, 1] = tot.reshape(n, HP, 128)

    for d in range(1, n):
        send(1, st_send.at[up(d, t)], st_recv.at[t], "tp", d, 1)
        send(1, o_send.at[up(d, t)], o_recv.at[t], "tp", d)
    o_recv[t] = o_send[t]
    st_recv[t] = st_send[t]
    for d in range(1, n):
        arrive(1, st_recv.at[down(d, t)], "tp", down(d, t), 1)
        arrive(1, o_recv.at[down(d, t)], "tp", down(d, t))
    ms = [st_recv[i, 0] for i in range(n)]
    best = functools.reduce(jnp.maximum, ms)
    es = [jnp.exp(m - best) for m in ms]
    total = sum(es[i] * st_recv[i, 1] for i in range(n))
    coef = [e / total for e in es]
    for b in range(rows):
        att[b] = sum(o_recv[i, b].astype(f32) * coef[i][:, b : b + 1] for i in range(n))
    for i in range(hc):
        attn_all[t, :, i * HD : (i + 1) * HD] = att[:, i, :].astype(bf16)

    for d in range(1, n):
        send(2, attn_all.at[t], attn_all.at[t], "tp", d)
    chunk_seen = {}
    for d in range(n):
        c = down(d, t)
        if d:
            arrive(2, attn_all.at[c], "tp", c)
    for d in range(1, n):
        send(3, attn_all.at[up(d, s)], attn_sub.at[s], "sub", d)
    attn_sub[s] = attn_all[s]
    for i in range(per_feat):
        ow_copy(i).wait()
    for d in range(1, n):
        arrive(3, attn_sub.at[down(d, s)], "sub", down(d, s))
    a = attn_sub[...].reshape(n * rows, feat)
    base = n_slots - per_feat
    proj = jnp.dot(a[:, :KC], slots[base, :, :feat], preferred_element_type=f32)
    for i in range(1, per_feat):
        proj += jnp.dot(
            a[:, i * KC : (i + 1) * KC], slots[base + i, :, :feat], preferred_element_type=f32
        )
    pr_send[...] = proj.astype(bf16).reshape(n, rows, feat)
    for i in range(min(per_feat, n_down)):
        down_copy(i).start()
    for d in range(1, n):
        send(4, pr_send.at[up(d, s)], pr_recv.at[s], "sub", d)
    pr_recv[s] = pr_send[s]
    for d in range(1, n):
        arrive(4, pr_recv.at[down(d, s)], "sub", down(d, s))
    res = hid_ref[...].astype(f32)
    for i in range(n):
        res += pr_recv[i].astype(f32)
    resid[...] = res
    hg = res * gain_ref[...]
    lane16 = lax.broadcasted_iota(jnp.int32, (rows, 128), 1)
    stat = jnp.where(lane16 == E, jnp.sum(res * res, axis=1, keepdims=True), 0.0)
    for e in range(E):
        part = jnp.sum(hg * rt_ref[e : e + 1, :], axis=1, keepdims=True)
        stat = jnp.where(lane16 == e, part, stat)
    hs_send[...] = stat
    x_all[t, s] = hg.astype(bf16)

    for d in range(1, n):
        send(5, hs_send, hs_recv.at[t], "tp", d, 1)
        send(5, x_all.at[t, s], x_all.at[t, s], "tp", d)
    for d in range(1, n):
        send(6, x_all.at[t, s], x_all.at[t, s], "sub", d, 0)
    hs_recv[t] = hs_send[...]
    for d in range(1, n):
        arrive(5, hs_recv.at[down(d, t)], "tp", down(d, t), 1)
    summed = sum(hs_recv[i] for i in range(n))
    rinv = lax.rsqrt(summed[:, E : E + 1] / (n * feat) + 1e-05)
    logits = summed * rinv
    first, second = routes_ref[:, 0:1], routes_ref[:, 1:2]
    first_hot, second_hot = lane16 == first, lane16 == second
    l1 = jnp.sum(jnp.where(first_hot, logits, 0.0), axis=1, keepdims=True)
    l2 = jnp.sum(jnp.where(second_hot, logits, 0.0), axis=1, keepdims=True)
    w1 = 1.0 / (1.0 + jnp.exp(l2 - l1))
    w2 = 1.0 / (1.0 + jnp.exp(l1 - l2))
    fin = jnp.where(first_hot, w1, 0.0) + jnp.where(second_hot, w2, 0.0)
    f_all[s] = jnp.where(lane16 == E, rinv, fin)
    for d in range(1, n):
        send(7, f_all.at[s], f_all.at[s], "sub", d)
    for j in range(1, n):
        c = down(j, t)
        arrive(5, x_all.at[c, s], "tp", c)
        for d in range(1, n):
            send(6, x_all.at[c, s], x_all.at[c, s], "sub", d, j)

    gacc[...] = jnp.zeros_like(gacc)
    uacc[...] = jnp.zeros_like(uacc)
    for block in range(n):
        c = up(block, t)
        j = (n - block) % n
        for d in range(1, n):
            arrive(6, x_all.at[c, down(d, s)], "sub", down(d, s), j)
        for part in range(per_feat):
            k = block * per_feat + part
            up_copy(gw_hbm, k, 0).wait()
            up_copy(uw_hbm, k, 1).wait()
            x = x_all[c, :, :, part * KC : (part + 1) * KC].reshape(n * rows, KC)
            gacc[...] += jnp.dot(x, slots[2 * k], preferred_element_type=f32)
            uacc[...] += jnp.dot(x, slots[2 * k + 1], preferred_element_type=f32)
            for j_down in (per_feat + 2 * k, per_feat + 2 * k + 1):
                if j_down < n_down:
                    down_copy(j_down).start()
    for d in range(1, n):
        arrive(7, f_all.at[down(d, s)], "sub", down(d, s))
    facts = f_all[...].reshape(n * rows, 128)
    rall = facts[:, E : E + 1]
    mine = lax.broadcasted_iota(jnp.int32, (n * rows, 128), 1) == s
    share = jnp.sum(jnp.where(mine, facts, 0.0), axis=1, keepdims=True)
    gate = gacc[...] * rall
    z = gate / (1.0 + jnp.exp(-gate)) * (uacc[...] * rall)
    inner[...] = z.astype(bf16)

    def settle(block):
        for d in range(1, n):
            who = down(d, s)
            arrive(8, y_recv.at[block, who], "sub", who, block)
        y = y_send[block, s].astype(f32)
        for d in range(1, n):
            y += y_recv[block, down(d, s)].astype(f32)
        if block < n - 1:
            z_send[block] = y.astype(bf16)
            send(9, z_send.at[block], z_recv.at[t], "tp", block + 1)
        return y

    for block in range(n):
        y = None
        for part in range(k_down):
            j = block * k_down + part
            down_copy(j).wait()
            slot = (j + n_slots - per_feat) % n_slots
            term = jnp.dot(
                inner[:, part * KC : (part + 1) * KC],
                slots[slot, :, :feat],
                preferred_element_type=f32,
            )
            y = term if y is None else y + term
        y_send[block] = (y * share).astype(bf16).reshape(n, rows, feat)
        for d in range(1, n):
            send(8, y_send.at[block, up(d, s)], y_recv.at[block, s], "sub", d, block)
        if block:
            settle(block - 1)
    result = resid[...] + settle(n - 1)
    for d in range(1, n):
        who = down(d, t)
        arrive(9, z_recv.at[who], "tp", who)
        result += z_recv[who].astype(f32)
    out_ref[...] = result.astype(bf16)
    for copy in pending:
        copy.wait_send()


def fused(n, hidden_in, query, key_new, value_new, key_cache, value_cache, lengths, out_weight,
          norm_gain, router_weight, routes, gate_weight, up_weight, down_weight):
    rows, feat = hidden_in.shape
    local_len = key_cache.shape[1]
    hc, kpc, group = feat // HD, KVH // n, H // KVH
    ff = gate_weight.shape[2]
    q3 = jnp.pad(query.reshape(rows, hc, HD), ((0, 0), (0, HP - hc), (0, 0)))
    kn3 = jnp.pad(key_new.reshape(rows, kpc, HD), ((0, 0), (0, HP - kpc), (0, 0)))
    vn3 = jnp.pad(value_new.reshape(rows, kpc, HD), ((0, 0), (0, HP - kpc), (0, 0)))
    head = np.arange(n * HP)
    chunk, inside = head // HP, head % HP
    real = inside < hc
    kv_of = np.where(real, chunk * kpc + inside // group, -1)
    lane = np.arange(KVH * local_len)
    kvm = (kv_of[:, None] == (lane // local_len)[None, :]).astype(np.float32)
    pos = (lane % local_len)[None, :].astype(np.int32)
    match = real[:, None] & ((inside // group)[:, None] == np.arange(HP)[None, :])
    own = np.where(match, chunk[:, None], -1).astype(np.int32)
    bf16, f32 = jnp.bfloat16, jnp.float32
    per_feat = feat // KC
    n_slots = 2 * n * per_feat + per_feat
    vm = pl.BlockSpec(memory_space=pltpu.VMEM)
    hbm = pl.BlockSpec(memory_space=pl.ANY)
    sm = pl.BlockSpec(memory_space=pltpu.SMEM)
    V = pltpu.VMEM
    return pl.pallas_call(
        functools.partial(layer_kernel, n),
        out_shape=jax.ShapeDtypeStruct((rows, feat), bf16),
        in_specs=[sm] + [vm] * 10 + [hbm] * 6,
        out_specs=vm,
        scratch_shapes=[
            V((n_slots, KC, ff), bf16),
            V((rows, local_len, KVH * HD), bf16),
            V((rows, local_len, KVH * HD), bf16),
            V((n, rows, HP, HD), bf16),
            V((n, rows, HP, HD), bf16),
            V((n, rows, HP, HD), bf16),
            V((n, 2, HP, 128), f32),
            V((n, 2, HP, 128), f32),
            V((rows, HP, HD), f32),
            V((n, rows, feat), bf16),
            V((n, rows, feat), bf16),
            V((n, rows, feat), bf16),
            V((n, rows, feat), bf16),
            V((rows, feat), f32),
            V((rows, 128), f32),
            V((n, rows, 128), f32),
            V((n, n, rows, feat), bf16),
            V((n, rows, 128), f32),
            V((n * rows, ff), f32),
            V((n * rows, ff), f32),
            V((n * rows, ff), bf16),
            V((n, n, rows, feat), bf16),
            V((n, n, rows, feat), bf16),
            V((n, rows, feat), bf16),
            V((n, rows, feat), bf16),
            pltpu.SemaphoreType.DMA((n_slots,)),
            pltpu.SemaphoreType.DMA((2,)),
            pltpu.SemaphoreType.DMA((10, n, n)),
            pltpu.SemaphoreType.DMA((10, n, n)),
        ],
        compiler_params=pltpu.CompilerParams(
            collective_id=0, has_side_effects=True, vmem_limit_bytes=67043328
        ),
    )(
        lengths, q3, kn3, vn3, hidden_in, norm_gain.astype(f32).reshape(1, feat),
        router_weight.astype(f32).T, routes, jnp.asarray(kvm), jnp.asarray(pos), jnp.asarray(own),
        key_cache, value_cache, out_weight, gate_weight, up_weight, down_weight,
    )


def pick(n_tp, n_sub, *args):
    rows, feat = args[0].shape
    ff = args[11].shape[2]
    whole_heads = feat % HD == 0 and KVH % n_tp == 0 and feat // HD <= HP
    tiles = rows % 16 == 0 and feat % KC == 0 and ff % KC == 0 and feat <= ff
    if n_tp == n_sub and whole_heads and tiles:
        return fused(n_tp, *args)
    return on_device(*args)


def solution(mesh):
    in_specs = (
        P(("rep", "sub"), "tp"),
        P(("rep", "sub"), "tp"),
        P(("rep", "sub"), "tp"),
        P(("rep", "sub"), "tp"),
        P(("rep", "sub"), "tp", None),
        P(("rep", "sub"), "tp", None),
        P(("rep", "sub")),
        P("sub", "tp"),
        P("tp"),
        P("tp", None),
        P(("rep", "sub"), None),
        P("sub", None, "tp"),
        P("sub", None, "tp"),
        P("sub", "tp", None),
    )
    out_specs = P(("rep", "sub"), "tp")
    return jax.shard_map(
        functools.partial(pick, mesh.shape["tp"], mesh.shape["sub"]), mesh=mesh, in_specs=in_specs, out_specs=out_specs, check_vma=False
    )
```

```python
import functools

import jax
import jax.numpy as jnp
import numpy as np
from jax import lax
from jax.experimental import pallas as pl
from jax.experimental.pallas import tpu as pltpu
from jax.sharding import PartitionSpec as P

D = 6144
H = 48
KVH = 8
HD = 128
E = 4


def combined_all(value, axis, combine):
    everything = jax.tree.map(lambda part: lax.all_gather(part, axis), value)
    first = jax.tree.map(lambda part: part[0], everything)

    def hop(k, so_far):
        return combine(so_far, jax.tree.map(lambda part: part[k], everything))

    return lax.fori_loop(1, lax.axis_size(axis), hop, first)


def join_softmax(first, second):
    joined = jnp.maximum(first[0], second[0])
    first_scale = jnp.exp(first[0] - joined)
    second_scale = jnp.exp(second[0] - joined)
    totals = first[1] * first_scale + second[1] * second_scale
    summed = first[2] * first_scale[..., None] + second[2] * second_scale[..., None]
    return (joined, totals, summed)


def on_device(
    hidden_in,
    query,
    key_new,
    value_new,
    key_cache,
    value_cache,
    lengths,
    out_weight,
    norm_gain,
    router_weight,
    routes,
    gate_weight,
    up_weight,
    down_weight,
):
    seq_rows = hidden_in.shape[0]
    feat_width = hidden_in.shape[1]
    group_size = H // KVH
    scale_factor = 1.0 / HD**0.5
    local_len = key_cache.shape[1]
    all_query, all_key, all_value = (
        lax.all_gather(query, "tp", axis=1, tiled=True),
        lax.all_gather(key_new, "tp", axis=1, tiled=True),
        lax.all_gather(value_new, "tp", axis=1, tiled=True),
    )
    query_rows = all_query.reshape(seq_rows, KVH, group_size, HD)
    cached_keys = key_cache.reshape(seq_rows, local_len, KVH, HD)
    cached_values = value_cache.reshape(seq_rows, local_len, KVH, HD).astype(jnp.float32)
    scores = (
        jnp.einsum("bkgd,bpkd->bkgp", query_rows, cached_keys, preferred_element_type=jnp.float32)
        * scale_factor
    )
    positions = lax.axis_index("tp") * local_len + jnp.arange(local_len, dtype=jnp.int32)
    valid = positions[None, :] < lengths[:, None]
    scores = jnp.where(valid[:, None, None, :], scores, -jnp.inf)
    owned_part = (
        jnp.einsum(
            "zyqn,zyn->zyq",
            query_rows,
            all_key.reshape(seq_rows, KVH, HD),
            preferred_element_type=jnp.float32,
        )
        * scale_factor
    )
    local_max = jnp.maximum(jnp.max(scores, axis=-1), owned_part)
    weights = jnp.exp(scores - local_max[..., None])
    partial_total = jnp.sum(weights, axis=-1)
    local_summed = jnp.einsum("bkgp,bpkd->bkgd", weights, cached_values)
    run_max, total, summed = combined_all(
        (local_max, partial_total, local_summed), "tp", join_softmax
    )
    own_weight = jnp.exp(owned_part - run_max)
    total = total + own_weight
    new_values = all_value.reshape(seq_rows, KVH, 1, HD).astype(jnp.float32)
    summed = summed + own_weight[..., None] * new_values
    attn = (summed / total[..., None]).reshape(seq_rows, H * HD).astype(jnp.bfloat16)
    all_rows_attn = lax.all_to_all(attn, "sub", split_axis=1, concat_axis=0, tiled=True)
    partial_proj = jnp.dot(all_rows_attn, out_weight, preferred_element_type=jnp.float32)
    projected = lax.psum_scatter(partial_proj, "sub", scatter_dimension=0, tiled=True)
    resid = hidden_in.astype(jnp.float32) + projected
    gain_full = norm_gain.astype(jnp.float32)[None, :]
    router_full = router_weight.astype(jnp.float32)
    squares = lax.psum(jnp.sum(resid * resid, axis=-1), "tp")
    root = jnp.sqrt(squares / D + 1e-05)
    normed = resid / root[:, None] * gain_full
    logits = lax.psum(jnp.dot(normed, router_full, precision=lax.Precision.HIGHEST), "tp")
    normed_low = normed.astype(jnp.bfloat16)
    expert_ids = jnp.arange(E, dtype=jnp.int32)[None, :]
    first_hot = (routes[:, 0:1] == expert_ids).astype(jnp.float32)
    second_hot = (routes[:, 1:2] == expert_ids).astype(jnp.float32)
    first_logit = jnp.sum(logits * first_hot, axis=-1)
    second_logit = jnp.sum(logits * second_hot, axis=-1)
    first_weight = 1.0 / (1.0 + jnp.exp(second_logit - first_logit))
    second_weight = 1.0 / (1.0 + jnp.exp(first_logit - second_logit))
    dense = first_weight[:, None] * first_hot + second_weight[:, None] * second_hot
    gate_local = gate_weight[0]
    up_local = up_weight[0]
    down_local = down_weight[0]
    every_row = lax.all_gather(normed_low, "sub", axis=0, tiled=True)
    piece = lax.all_gather(every_row, "tp", axis=1, tiled=True)
    gate_out = jnp.dot(piece, gate_local, preferred_element_type=jnp.float32)
    up_out = jnp.dot(piece, up_local, preferred_element_type=jnp.float32)
    inner = (jax.nn.silu(gate_out) * up_out).astype(jnp.bfloat16)
    result = jnp.dot(inner, down_local, preferred_element_type=jnp.float32)
    outputs = lax.psum_scatter(result, "tp", scatter_dimension=1, tiled=True)
    returned = lax.all_to_all(outputs, "sub", split_axis=0, concat_axis=0, tiled=True)
    returned = returned.reshape(E, seq_rows, feat_width)
    mixed = jnp.einsum("erc,re->rc", returned, dense)
    return (resid + mixed).astype(jnp.bfloat16)


MESH = pl.DeviceIdType.MESH
HP = 16
KC = 512
HALF = 64
NEG = -1e30


def layer_kernel(
    n,
    len_ref, q_ref, kn_ref, vn_ref, hid_ref, gain_ref, rt_ref, routes_ref, kvm_ref, pos_ref, own_ref,
    kc_hbm, vc_hbm, ow_hbm, gw_hbm, uw_hbm, dw_hbm,
    out_ref,
    slots, kc, vc, q_all, o_send, o_recv, st_send, st_recv, att, attn_all, attn_sub,
    qf, knf, vnf, pr_send, pr_recv, resid, hs_send, hs_recv, x_all, f_all, gacc, uacc, inner,
    y_send, y_recv, z_send, z_recv,
    slot_sem, kv_sem, send_sem, recv_sem,
):
    t = lax.axis_index("tp")
    s = lax.axis_index("sub")
    rows, feat = hid_ref.shape
    local_len = kc.shape[1]
    kvh = kc.shape[2] // HD
    hc = feat // HD
    ff = slots.shape[2]
    n_slots = slots.shape[0]
    per_feat = feat // KC
    n_up = n * per_feat
    k_down = ff // KC
    n_down = n * k_down
    f32, bf16 = jnp.float32, jnp.bfloat16

    def up(d, i):
        return lax.rem(i + d, n)

    def down(d, i):
        return lax.rem(i + n - d, n)

    barrier = pltpu.get_barrier_semaphore()
    for d in range(1, n):
        pl.semaphore_signal(barrier, inc=1, device_id={"tp": up(d, t)}, device_id_type=MESH)
        pl.semaphore_signal(barrier, inc=1, device_id={"sub": up(d, s)}, device_id_type=MESH)

    kcopy = pltpu.make_async_copy(kc_hbm, kc, kv_sem.at[0])
    vcopy = pltpu.make_async_copy(vc_hbm, vc, kv_sem.at[1])
    kcopy.start()
    vcopy.start()

    def ow_copy(i):
        slot = n_slots - per_feat + i
        return pltpu.make_async_copy(
            ow_hbm.at[pl.ds(i * KC, KC), :], slots.at[slot, :, pl.ds(0, feat)], slot_sem.at[slot]
        )

    def up_copy(hbm, k, which):
        block, part = k // per_feat, lax.rem(k, per_feat)
        row = pl.multiple_of(up(block, t) * feat + part * KC, KC)
        return pltpu.make_async_copy(
            hbm.at[0, pl.ds(row, KC), :], slots.at[2 * k + which], slot_sem.at[2 * k + which]
        )

    def down_copy(j):
        block, part = j // k_down, lax.rem(j, k_down)
        slot = lax.rem(j + n_slots - per_feat, n_slots)
        col = pl.multiple_of(up(block + 1, t) * feat, 128)
        row = pl.multiple_of(part * KC, KC)
        return pltpu.make_async_copy(
            dw_hbm.at[0, pl.ds(row, KC), pl.ds(col, feat)],
            slots.at[slot, :, pl.ds(0, feat)],
            slot_sem.at[slot],
        )

    for i in range(per_feat):
        ow_copy(i).start()

    @pl.loop(0, n_up)
    def _(k):
        up_copy(gw_hbm, k, 0).start()
        up_copy(uw_hbm, k, 1).start()

    pl.semaphore_wait(barrier, 2 * (n - 1))

    def remote(stage, source, target, axis, peer, key, lane, who):
        return pltpu.make_async_remote_copy(
            src_ref=source,
            dst_ref=target,
            send_sem=send_sem.at[stage, key, lane],
            recv_sem=recv_sem.at[stage, who, lane],
            device_id={axis: peer},
            device_id_type=MESH,
        )

    pending = []

    def send(stage, source, target, axis, d, lane=0):
        me = t if axis == "tp" else s
        copy = remote(stage, source, target, axis, up(d, me), d, lane, me)
        copy.start()
        pending.append(copy)

    def arrive(stage, target, axis, who, lane=0):
        remote(stage, target, target, axis, who, 0, lane, who).wait_recv()

    for d in range(1, n):
        send(0, q_ref, q_all.at[t], "tp", d)
    qf[...] = jnp.zeros_like(qf)
    knf[...] = jnp.zeros_like(knf)
    vnf[...] = jnp.zeros_like(vnf)
    for i in range(kn_ref.shape[1] // HD):
        knf[:, i, :] = kn_ref[:, i * HD : (i + 1) * HD].astype(f32)
        vnf[:, i, :] = vn_ref[:, i * HD : (i + 1) * HD].astype(f32)
    q_all[t] = q_ref[...]
    for d in range(n):
        c = down(d, t)
        if d:
            arrive(0, q_all.at[c], "tp", c)
        for i in range(hc):
            qf[c, :, i, :] = q_all[c, :, i * HD : (i + 1) * HD].astype(f32)
    kcopy.wait()
    vcopy.wait()

    lanes = lax.broadcasted_iota(jnp.int32, (n * HP, 128), 1)
    scale = 1.0 / HD**0.5
    kvm = kvm_ref[...] > 0.5
    positions = pos_ref[...] + t * local_len
    own_ok = own_ref[...] == t

    def per_row(b, stats):
        q = qf[:, b].reshape(n * HP, HD).astype(bf16)
        krow, vrow = kc[b], vc[b]
        keys = jnp.concatenate([krow[:, g * HD : (g + 1) * HD] for g in range(kvh)], axis=0)
        vals = jnp.concatenate([vrow[:, g * HD : (g + 1) * HD] for g in range(kvh)], axis=0)
        dims = (((1,), (1,)), ((), ()))
        sc = lax.dot_general(q, keys, dims, preferred_element_type=f32) * scale
        so = lax.dot_general(q, knf[b].astype(bf16), dims, preferred_element_type=f32) * scale
        ok = jnp.logical_and(kvm, positions < len_ref[b])
        sc = jnp.where(ok, sc, NEG)
        so = jnp.where(own_ok, so, NEG)
        m = jnp.maximum(jnp.max(sc, axis=1, keepdims=True), jnp.max(so, axis=1, keepdims=True))
        p = jnp.where(ok, jnp.exp(sc - m), 0.0)
        po = jnp.where(own_ok, jnp.exp(so - m), 0.0)
        l = jnp.sum(p, axis=1, keepdims=True) + jnp.sum(po, axis=1, keepdims=True)
        o = jnp.dot(p.astype(bf16), vals, preferred_element_type=f32)
        o = o + jnp.dot(po.astype(bf16), vnf[b].astype(bf16), preferred_element_type=f32)
        o_send[:, b] = o.astype(bf16).reshape(n, HP, HD)
        return jnp.where(lanes == b, m, jnp.where(lanes == b + HALF, l, stats))

    zero = jnp.zeros((n * HP, 128), f32)
    stats = lax.fori_loop(0, rows, per_row, zero, unroll=4)
    st_send[...] = stats.reshape(n, HP, 128)

    for d in range(1, n):
        send(1, st_send.at[up(d, t)], st_recv.at[t], "tp", d, 1)
        send(1, o_send.at[up(d, t)], o_recv.at[t], "tp", d)
    o_recv[t] = o_send[t]
    st_recv[t] = st_send[t]
    for d in range(1, n):
        arrive(1, st_recv.at[down(d, t)], "tp", down(d, t), 1)
        arrive(1, o_recv.at[down(d, t)], "tp", down(d, t))
    ms = [st_recv[i] for i in range(n)]
    best = functools.reduce(jnp.maximum, ms)
    es = [jnp.exp(m - best) for m in ms]
    total = sum(es[i] * pltpu.roll(ms[i], HALF, 1) for i in range(n))
    coef = [e / total for e in es]
    for b in range(rows):
        att[b] = sum(o_recv[i, b].astype(f32) * coef[i][:, b : b + 1] for i in range(n))
    for i in range(hc):
        attn_all[t, :, i * HD : (i + 1) * HD] = att[:, i, :].astype(bf16)

    for d in range(1, n):
        send(2, attn_all.at[t], attn_all.at[t], "tp", d)

    def onward(c):
        return remote(3, attn_all.at[c], attn_sub.at[s], "sub", c, c, 0, s)

    for d in range(n):
        c = down(d, t)
        if d:
            arrive(2, attn_all.at[c], "tp", c)

        @pl.when(c != s)
        def _():
            onward(c).start()

    attn_sub[s] = attn_all[s]
    for i in range(per_feat):
        ow_copy(i).wait()
    for d in range(1, n):
        arrive(3, attn_sub.at[down(d, s)], "sub", down(d, s))
    a = attn_sub[...].reshape(n * rows, feat)
    base = n_slots - per_feat
    proj = jnp.dot(a[:, :KC], slots[base, :, :feat], preferred_element_type=f32)
    for i in range(1, per_feat):
        proj += jnp.dot(
            a[:, i * KC : (i + 1) * KC], slots[base + i, :, :feat], preferred_element_type=f32
        )
    pr_send[...] = proj.astype(bf16).reshape(n, rows, feat)
    for i in range(min(per_feat, n_down)):
        down_copy(i).start()
    for d in range(1, n):
        send(4, pr_send.at[up(d, s)], pr_recv.at[s], "sub", d)
    pr_recv[s] = pr_send[s]
    for d in range(1, n):
        arrive(4, pr_recv.at[down(d, s)], "sub", down(d, s))
    res = hid_ref[...].astype(f32)
    for i in range(n):
        res += pr_recv[i].astype(f32)
    resid[...] = res
    hg = res * gain_ref[...].astype(f32).reshape(1, feat)
    lane16 = lax.broadcasted_iota(jnp.int32, (rows, 128), 1)
    stat = jnp.where(lane16 == E, jnp.sum(res * res, axis=1, keepdims=True), 0.0)
    for e in range(E):
        part = jnp.sum(hg * rt_ref[e : e + 1, :].astype(f32), axis=1, keepdims=True)
        stat = jnp.where(lane16 == e, part, stat)
    hs_send[...] = stat
    x_all[t, s] = hg.astype(bf16)

    for d in range(1, n):
        send(5, hs_send, hs_recv.at[t], "tp", d, 1)
        send(5, x_all.at[t, s], x_all.at[t, s], "tp", d)
    for d in range(1, n):
        send(6, x_all.at[t, s], x_all.at[t, s], "sub", d, 0)
    hs_recv[t] = hs_send[...]
    for d in range(1, n):
        arrive(5, hs_recv.at[down(d, t)], "tp", down(d, t), 1)
    summed = sum(hs_recv[i] for i in range(n))
    rinv = lax.rsqrt(summed[:, E : E + 1] / (n * feat) + 1e-05)
    logits = summed * rinv
    square = (rows, rows)
    eye = lax.broadcasted_iota(jnp.int32, square, 0) == lax.broadcasted_iota(jnp.int32, square, 1)

    def column(i):
        row = routes_ref[i : i + 1, :].astype(f32)
        return jnp.sum(jnp.where(eye, row, 0.0), axis=1, keepdims=True).astype(jnp.int32)

    first, second = column(0), column(1)
    first_hot, second_hot = lane16 == first, lane16 == second
    l1 = jnp.sum(jnp.where(first_hot, logits, 0.0), axis=1, keepdims=True)
    l2 = jnp.sum(jnp.where(second_hot, logits, 0.0), axis=1, keepdims=True)
    w1 = 1.0 / (1.0 + jnp.exp(l2 - l1))
    w2 = 1.0 / (1.0 + jnp.exp(l1 - l2))
    fin = jnp.where(first_hot, w1, 0.0) + jnp.where(second_hot, w2, 0.0)
    f_all[s] = jnp.where(lane16 == E, rinv, fin)
    for d in range(1, n):
        send(7, f_all.at[s], f_all.at[s], "sub", d)
    for j in range(1, n):
        c = down(j, t)
        arrive(5, x_all.at[c, s], "tp", c)
        for d in range(1, n):
            send(6, x_all.at[c, s], x_all.at[c, s], "sub", d, j)

    gacc[...] = jnp.zeros_like(gacc)
    uacc[...] = jnp.zeros_like(uacc)
    for block in range(n):
        c = up(block, t)
        j = (n - block) % n
        for d in range(1, n):
            arrive(6, x_all.at[c, down(d, s)], "sub", down(d, s), j)
        for part in range(per_feat):
            k = block * per_feat + part
            up_copy(gw_hbm, k, 0).wait()
            up_copy(uw_hbm, k, 1).wait()
            x = x_all[c, :, :, part * KC : (part + 1) * KC].reshape(n * rows, KC)
            gacc[...] += jnp.dot(x, slots[2 * k], preferred_element_type=f32)
            uacc[...] += jnp.dot(x, slots[2 * k + 1], preferred_element_type=f32)
            for j_down in (per_feat + 2 * k, per_feat + 2 * k + 1):
                if j_down < n_down:
                    down_copy(j_down).start()
    for d in range(1, n):
        arrive(7, f_all.at[down(d, s)], "sub", down(d, s))
    facts = f_all[...].reshape(n * rows, 128)
    rall = facts[:, E : E + 1]
    mine = lax.broadcasted_iota(jnp.int32, (n * rows, 128), 1) == s
    share = jnp.sum(jnp.where(mine, facts, 0.0), axis=1, keepdims=True)
    gate = gacc[...] * rall
    z = gate / (1.0 + jnp.exp(-gate)) * (uacc[...] * rall)
    inner[...] = z.astype(bf16)

    def settle(block):
        for d in range(1, n):
            who = down(d, s)
            arrive(8, y_recv.at[block, who], "sub", who, block)
        y = y_send[block, s].astype(f32)
        for d in range(1, n):
            y += y_recv[block, down(d, s)].astype(f32)
        if block < n - 1:
            z_send[block] = y.astype(bf16)
            send(9, z_send.at[block], z_recv.at[t], "tp", block + 1)
        return y

    for block in range(n):
        y = None
        for part in range(k_down):
            j = block * k_down + part
            down_copy(j).wait()
            slot = (j + n_slots - per_feat) % n_slots
            term = jnp.dot(
                inner[:, part * KC : (part + 1) * KC],
                slots[slot, :, :feat],
                preferred_element_type=f32,
            )
            y = term if y is None else y + term
        y_send[block] = (y * share).astype(bf16).reshape(n, rows, feat)
        for d in range(1, n):
            send(8, y_send.at[block, up(d, s)], y_recv.at[block, s], "sub", d, block)
        if block:
            settle(block - 1)
    result = resid[...] + settle(n - 1)
    for d in range(1, n):
        who = down(d, t)
        arrive(9, z_recv.at[who], "tp", who)
        result += z_recv[who].astype(f32)
    out_ref[...] = result.astype(bf16)
    for d in range(1, n):
        onward(up(d, s)).wait_send()
    for copy in pending:
        copy.wait_send()


def fused(n, hidden_in, query, key_new, value_new, key_cache, value_cache, lengths, out_weight,
          norm_gain, router_weight, routes, gate_weight, up_weight, down_weight):
    rows, feat = hidden_in.shape
    local_len = key_cache.shape[1]
    hc, kpc, group = feat // HD, KVH // n, H // KVH
    ff = gate_weight.shape[2]
    head = np.arange(n * HP)
    chunk, inside = head // HP, head % HP
    real = inside < hc
    kv_of = np.where(real, chunk * kpc + inside // group, -1)
    lane = np.arange(KVH * local_len)
    kvm = (kv_of[:, None] == (lane // local_len)[None, :]).astype(np.float32)
    pos = (lane % local_len)[None, :].astype(np.int32)
    match = real[:, None] & ((inside // group)[:, None] == np.arange(HP)[None, :])
    own = np.where(match, chunk[:, None], -1).astype(np.int32)
    bf16, f32 = jnp.bfloat16, jnp.float32
    per_feat = feat // KC
    n_slots = 2 * n * per_feat + per_feat
    vm = pl.BlockSpec(memory_space=pltpu.VMEM)
    hbm = pl.BlockSpec(memory_space=pl.ANY)
    sm = pl.BlockSpec(memory_space=pltpu.SMEM)
    V = pltpu.VMEM
    return pl.pallas_call(
        functools.partial(layer_kernel, n),
        out_shape=jax.ShapeDtypeStruct((rows, feat), bf16),
        in_specs=[sm] + [vm] * 10 + [hbm] * 6,
        out_specs=vm,
        scratch_shapes=[
            V((n_slots, KC, ff), bf16),
            V((rows, local_len, KVH * HD), bf16),
            V((rows, local_len, KVH * HD), bf16),
            V((n, rows, feat), bf16),
            V((n, rows, HP, HD), bf16),
            V((n, rows, HP, HD), bf16),
            V((n, HP, 128), f32),
            V((n, HP, 128), f32),
            V((rows, HP, HD), f32),
            V((n, rows, feat), bf16),
            V((n, rows, feat), bf16),
            V((n, rows, HP, HD), f32),
            V((rows, HP, HD), f32),
            V((rows, HP, HD), f32),
            V((n, rows, feat), bf16),
            V((n, rows, feat), bf16),
            V((rows, feat), f32),
            V((rows, 128), f32),
            V((n, rows, 128), f32),
            V((n, n, rows, feat), bf16),
            V((n, rows, 128), f32),
            V((n * rows, ff), f32),
            V((n * rows, ff), f32),
            V((n * rows, ff), bf16),
            V((n, n, rows, feat), bf16),
            V((n, n, rows, feat), bf16),
            V((n, rows, feat), bf16),
            V((n, rows, feat), bf16),
            pltpu.SemaphoreType.DMA((n_slots,)),
            pltpu.SemaphoreType.DMA((2,)),
            pltpu.SemaphoreType.DMA((10, n, n)),
            pltpu.SemaphoreType.DMA((10, n, n)),
        ],
        compiler_params=pltpu.CompilerParams(
            collective_id=0, has_side_effects=True, vmem_limit_bytes=67043328
        ),
    )(
        lengths, query, key_new, value_new, hidden_in, norm_gain,
        router_weight.T, routes.T, jnp.asarray(kvm), jnp.asarray(pos), jnp.asarray(own),
        key_cache, value_cache, out_weight, gate_weight, up_weight, down_weight,
    )


def pick(n_tp, n_sub, *args):
    rows, feat = args[0].shape
    ff = args[11].shape[2]
    whole_heads = feat % HD == 0 and KVH % n_tp == 0 and feat // HD <= HP
    tiles = rows % 16 == 0 and rows <= HALF and feat % KC == 0 and ff % KC == 0 and feat <= ff
    if n_tp == n_sub and whole_heads and tiles:
        return fused(n_tp, *args)
    return on_device(*args)


def solution(mesh):
    in_specs = (
        P(("rep", "sub"), "tp"),
        P(("rep", "sub"), "tp"),
        P(("rep", "sub"), "tp"),
        P(("rep", "sub"), "tp"),
        P(("rep", "sub"), "tp", None),
        P(("rep", "sub"), "tp", None),
        P(("rep", "sub")),
        P("sub", "tp"),
        P("tp"),
        P("tp", None),
        P(("rep", "sub"), None),
        P("sub", None, "tp"),
        P("sub", None, "tp"),
        P("sub", "tp", None),
    )
    out_specs = P(("rep", "sub"), "tp")
    return jax.shard_map(
        functools.partial(pick, mesh.shape["tp"], mesh.shape["sub"]), mesh=mesh, in_specs=in_specs, out_specs=out_specs, check_vma=False
    )
```
